64 devices in a mesh: rep: 8 (over x, y, core), dp: 8 (over z).
Axes of the slice: x: 2, y: 2, z: 8, core: 2. Of those that a mesh axis runs over, the one named last changes fastest.
The devices are a block of a 4x4x8 slice.
Arguments:
- x: bfloat16 [64, 2048, 512], P(('rep', 'dp')), parts along dimension 0
- dy: bfloat16 [64, 2048, 512], P(('rep', 'dp')), parts along dimension 0
- w_gate: bfloat16 [2, 512, 2048], P(None, 'dp')
- w_up: bfloat16 [2, 512, 2048], P(None, 'dp')
- w_down: bfloat16 [2, 2048, 512], P(None, 'dp')
- m_w_gate: float32 [2, 512, 2048], P(None, 'dp')
- m_w_up: float32 [2, 512, 2048], P(None, 'dp')
- m_w_down: float32 [2, 2048, 512], P(None, 'dp')
- v_w_gate: float32 [2, 512, 2048], P(None, 'dp')
- v_w_up: float32 [2, 512, 2048], P(None, 'dp')
- v_w_down: float32 [2, 2048, 512], P(None, 'dp')
Outputs:
- output 1: bfloat16 [16, 512, 2048], P('rep', 'dp'), parts along dimension 0
- output 2: bfloat16 [16, 512, 2048], P('rep', 'dp'), parts along dimension 0
- output 3: bfloat16 [16, 2048, 512], P('rep', 'dp'), parts along dimension 0
- output 4: float32 [16, 512, 2048], P('rep', 'dp'), parts along dimension 0
- output 5: float32 [16, 512, 2048], P('rep', 'dp'), parts along dimension 0
- output 6: float32 [16, 2048, 512], P('rep', 'dp'), parts along dimension 0
- output 7: float32 [16, 512, 2048], P('rep', 'dp'), parts along dimension 0
- output 8: float32 [16, 512, 2048], P('rep', 'dp'), parts along dimension 0
- output 9: float32 [16, 2048, 512], P('rep', 'dp'), parts along dimension 0
There are 8 independent parts. The reference program is written for one: setup_inputs(seed, part) draws one part's arguments, and reference() takes and returns one part's arrays. A program takes and returns all parts, laid end to end along the dimension named above; an argument that names none is the same for every part.
All inputs are finite; a program needn't handle non-finite values.
Results may differ from the reference program's by a relative error of at most 0.022.
Values are sent between devices in bfloat16 or wider.
A program may use at most 768 MiB of HBM per device.

```python
import jax
import jax.numpy as jnp
from jax import lax

SEQUENCES = 8
TOKENS = 2048
D = 512
FF = 2048
LAYERS = 2
NAMES = ("w_gate", "w_up", "w_down")
SHAPES = {"w_gate": (LAYERS, D, FF), "w_up": (LAYERS, D, FF), "w_down": (LAYERS, FF, D)}


def bump(key, n, height):
    away = (jnp.arange(n, dtype=jnp.int32) - jax.random.randint(key, (), 0, n, jnp.int32)) % n
    return jnp.where(away < n // 8, height, 1.0)


def together(key, own, strength):
    shared = jax.random.normal(key, own.shape[1:], jnp.float32)
    return (own + strength * shared) * lax.rsqrt(1 + strength * strength)


def setup_inputs(seed: int = 0, part: int = 0) -> dict:
    kx, kdy, ka, kb, kz, kf, kh, kl, *keys = jax.random.split(jax.random.key(seed), 8 + 3 * len(NAMES))
    kx, kdy, ka, kb = (jax.random.fold_in(k, part) for k in (kx, kdy, ka, kb))
    kw, km, kv = (keys[i::3] for i in range(3))
    shape = (SEQUENCES, TOKENS, D)
    much_x, much_dy = jax.random.uniform(kz, (2,), jnp.float32, 0.0, 1.0)
    loud = 2.0 ** jax.random.uniform(jax.random.fold_in(kz, 1), (), jnp.float32, -1.0, 2.0)
    layers = 2.0 ** jax.random.uniform(kl, (LAYERS, 1, 1), jnp.float32, -1.0, 1.0)
    x = together(ka, jax.random.normal(kx, shape, jnp.float32), much_x) * bump(kf, D, 4.0)
    dy = together(kb, jax.random.normal(kdy, shape, jnp.float32), much_dy)
    drawn = {"x": x.astype(jnp.bfloat16), "dy": (loud * dy * (SEQUENCES * TOKENS) ** -0.5).astype(jnp.bfloat16)}
    for key, name in zip(kw, NAMES, strict=True):
        w = jax.random.normal(key, SHAPES[name], jnp.float32) * SHAPES[name][1] ** -0.5
        drawn[name] = (w * {"w_gate": 1.0, "w_up": bump(kh, FF, 4.0), "w_down": layers}[name]).astype(jnp.bfloat16)
    for key, name in zip(km, NAMES, strict=True):
        drawn[f"m_{name}"] = 0.1 * jax.random.normal(key, SHAPES[name], jnp.float32)
    for key, name in zip(kv, NAMES, strict=True):
        drawn[f"v_{name}"] = jax.random.uniform(key, SHAPES[name], jnp.float32, 0.005, 0.015)
    return drawn


def matmul(a, w):
    return jnp.dot(a, w, preferred_element_type=jnp.float32).astype(jnp.bfloat16)


def normed(h):
    wide = h.astype(jnp.float32)
    scale = lax.rsqrt(jnp.mean(wide**2, -1, keepdims=True) + 1e-6)
    return (wide * scale).astype(jnp.bfloat16)


def layer(h, w):
    a = normed(h)
    gate = jnp.dot(a, w["w_gate"], preferred_element_type=jnp.float32)
    up = jnp.dot(a, w["w_up"], preferred_element_type=jnp.float32)
    return h + matmul((jax.nn.silu(gate) * up).astype(jnp.bfloat16), w["w_down"])


def adamw(w, m, v, g):
    m = 0.9 * m + 0.1 * g
    v = 0.95 * v + 0.05 * g * g
    step = m * lax.rsqrt(v + 1e-8) + 0.1 * w
    return (w - 0.02 * step).astype(jnp.bfloat16), m, v


def clipped(gradients, sum_of_squares, count):
    factor = jnp.minimum(1.0, 0.5 * lax.rsqrt(sum_of_squares / count + 1e-30))
    return [g * factor for g in gradients]


def stack(weights, h):
    return lax.scan(lambda h, w: (layer(h, w), None), h, weights)[0]


def reference(x, dy, w_gate, w_up, w_down, m_w_gate, m_w_up, m_w_down, v_w_gate, v_w_up, v_w_down):
    weights = dict(zip(NAMES, (w_gate, w_up, w_down), strict=True))

    def take(so_far, sequence):
        h, by_y = sequence
        _, back = jax.vjp(lambda w: stack(w, h), weights)
        return jax.tree.map(lambda total, term: total + term.astype(jnp.float32), so_far, back(by_y)[0]), None

    none_yet = {name: jnp.zeros(w.shape, jnp.float32) for name, w in weights.items()}
    by_weights, _ = lax.scan(take, none_yet, (x, dy))
    gradients = [by_weights[name].astype(jnp.bfloat16).astype(jnp.float32) for name in NAMES]
    gradients = clipped(gradients, sum(jnp.sum(g * g) for g in gradients), sum(g.size for g in gradients))
    new = [
        adamw(w.astype(jnp.float32), m, v, g)
        for w, m, v, g in zip((w_gate, w_up, w_down), (m_w_gate, m_w_up, m_w_down), (v_w_gate, v_w_up, v_w_down), gradients, strict=True)
    ]
    return tuple(one[which] for which in range(3) for one in new)
```

```python
import functools
import math

import jax
import jax.numpy as jnp
from jax import lax
from jax.experimental import pallas as pl
from jax.experimental.pallas import tpu as pltpu
from jax.sharding import PartitionSpec as P

MESH = pl.DeviceIdType.MESH
F32, BF16 = jnp.float32, jnp.bfloat16
CHUNKS = 4
SPACING = 4
PHASE = 8


def dot(a, b):
    return jnp.dot(a, b, preferred_element_type=F32)


def dot_t(a, b):
    return lax.dot_general(a, b, (((1,), (1,)), ((), ())), preferred_element_type=F32)


def sigmoid(x):
    return 0.5 * jnp.tanh(0.5 * x) + 0.5


def scale_of(wide):
    return lax.rsqrt(jnp.mean(wide * wide, -1, keepdims=True) + 1e-6)


def span(start, size):
    return pl.ds(pl.multiple_of(start, size), size)


def kernel(
    n,
    across,
    x_in,
    dy_in,
    wg_in,
    wu_in,
    wd_in,
    gu_out,
    gd_out,
    factor_out,
    wgu,
    wd,
    gu,
    gd,
    land_gu,
    land_gd,
    xs,
    do,
    h1,
    a,
    at,
    dot_do,
    big,
    acc,
    squares_gu,
    squares_gd,
    all_squares,
    load_sem,
    out_sem,
    ag_send,
    ag_z,
    ag_pair,
    ag_core,
    rs_send,
    rs_recv,
    sq_send,
    sq_recv,
):
    tokens, d = xs.shape
    ff = wgu.shape[3]
    own_d, own_f = d // n, ff // n
    fc = ff // CHUNKS
    me, rep = lax.axis_index("dp"), lax.axis_index("rep")
    core, y_bit, x_bit = rep % 2, (rep // 2) % 2, (rep // (2 * across)) % 2
    parity = (x_bit + y_bit) % 2

    def around(k):
        return lax.rem(me + (k + n), n)

    right, left = {"dp": around(1)}, {"dp": around(-1)}
    other_core = {"rep": rep + 1 - 2 * core}
    other_y = {"rep": rep + 2 - 4 * y_bit}
    other_x = {"rep": rep + 2 * across * (1 - 2 * x_bit)}

    barrier = pltpu.get_barrier_semaphore()
    partners = [{"dp": around(k)} for k in range(1, n)] + [other_core, other_y, other_x]
    for partner in partners:
        pl.semaphore_signal(barrier, inc=1, device_id=partner, device_id_type=MESH)

    loads = []
    for number in range(2):
        loads.append(pltpu.make_async_copy(wg_in.at[number], wgu.at[number, 0, span(me * own_d, own_d), :], load_sem.at[number, 0]))
        loads.append(pltpu.make_async_copy(wu_in.at[number], wgu.at[number, 1, span(me * own_d, own_d), :], load_sem.at[number, 1]))
        loads.append(pltpu.make_async_copy(wd_in.at[number], wd.at[number, span(me * own_f, own_f), :], load_sem.at[number, 2]))
    load_x = pltpu.make_async_copy(x_in.at[0], xs, load_sem.at[0, 3])
    load_dy = pltpu.make_async_copy(dy_in.at[0], do, load_sem.at[1, 3])
    for load in loads[:3] + [load_x] + loads[3:] + [load_dy]:
        load.start()
    pl.semaphore_wait(barrier, len(partners))

    eighth_f, eighth_r = ff // 8, own_f // 8
    mine = 4 * core + 2 * parity
    theirs = 4 * core + 2 * (1 - parity)

    def part(kind, number, shard, eighth, count):
        if kind == 0:
            return wgu.at[number, :, span(shard * own_d, own_d), pl.ds(pl.multiple_of(eighth * eighth_f, eighth_f), count * eighth_f)]
        return wd.at[number, pl.ds(pl.multiple_of(shard * own_f + eighth * eighth_r, eighth_r), count * eighth_r), :]

    def bytes_of(kind, number, eighths):
        if kind == 0:
            return wgu.at[number, :, pl.ds(0, eighths * own_d // 8), :]
        return wd.at[number, pl.ds(0, eighths * eighth_r), :]

    def await_eighths(kind, number, eighths, sem):
        ref = bytes_of(kind, number, eighths)
        pltpu.make_async_copy(ref, ref, sem).wait()

    def push(kind, number, shard, eighth, count, recv_sem, device):
        ref = part(kind, number, shard, eighth, count)
        pltpu.make_async_remote_copy(
            src_ref=ref, dst_ref=ref, send_sem=ag_send.at[kind, number], recv_sem=recv_sem, device_id=device, device_id_type=MESH
        ).start()

    def gather_round(kind, number, r):
        core_sem = ag_core.at[kind, number]
        if r >= 1 and r <= 4:
            await_eighths(kind, number, 4 if r <= 3 else 2, ag_z.at[kind, number, r - 1])
        if r <= 2:
            push(kind, number, around(-r), mine, 2, ag_z.at[kind, number, r], right)
            push(kind, number, around(r), mine, 2, ag_z.at[kind, number, r], left)
        elif r == 3:
            push(kind, number, around(-r), mine, 1, ag_z.at[kind, number, r], right)
            push(kind, number, around(r), mine + 1, 1, ag_z.at[kind, number, r], left)
        if r >= 1 and r <= 4:
            for shard in (around(-r), around(r)) if r <= 3 else (around(r),):
                push(kind, number, shard, mine, 1, ag_pair.at[kind, number, r - 1], other_y)
                push(kind, number, shard, mine + 1, 1, ag_pair.at[kind, number, r - 1], other_x)
                push(kind, number, shard, mine, 2, core_sem, other_core)
        if r >= 2:
            s = r - 1
            await_eighths(kind, number, 4 if s <= 3 else 2, ag_pair.at[kind, number, s - 1])
            for shard in (around(-s), around(s)) if s <= 3 else (around(s),):
                push(kind, number, shard, theirs, 2, core_sem, other_core)

    def gathered(kind, number):
        await_eighths(kind, number, 28, ag_core.at[kind, number])

    half_d = own_d // 2
    rows_d = d // 2
    half_r = rows_d // 2
    sides = ((right, 1), (left, -1))

    def wait_for(ref, sem):
        pltpu.make_async_copy(ref, ref, sem).wait()

    def hop(lam, q, s, group, block_of, half_of, slot_of, slot_half_of, final):
        for side, (device, sign) in enumerate(sides):
            send, recv = rs_send.at[group, side], rs_recv.at[group, side]
            block = lax.rem(me + sign * (4 - s) + n, n)

            def go(src, dst, step, send=send, recv=recv, device=device):
                pltpu.make_async_remote_copy(
                    src_ref=src, dst_ref=dst, send_sem=send, recv_sem=recv.at[step], device_id=device, device_id_type=MESH
                ).start()

            @pl.when(s == 0)
            def _(side=side, block=block, go=go):
                go(half_of(block, side), slot_half_of(side, 0, side), 0)

            @pl.when(s == 1)
            def _(side=side, block=block, go=go, send=send, recv=recv):
                wait_for(slot_half_of(side, 0, side), send)
                wait_for(slot_half_of(side, 0, side), recv.at[0])
                total, arrived = half_of(block, side), slot_half_of(side, 0, side)
                total[...] = (total[...].astype(F32) + arrived[...].astype(F32)).astype(BF16)
                go(block_of(block), slot_of(side, 1), 1)

            @pl.when((s == 2) | (s == 3))
            def _(side=side, block=block, go=go, send=send, recv=recv):
                wait_for(slot_of(side, s - 1), send)
                wait_for(slot_of(side, s - 1), recv.at[s - 1])
                total, arrived = block_of(block), slot_of(side, s - 1)
                total[...] = (total[...].astype(F32) + arrived[...].astype(F32)).astype(BF16)
                go(block_of(block), slot_of(side, s), s)

        @pl.when(s == 4)
        def _():
            for side in range(2):
                wait_for(slot_of(side, 3), rs_send.at[group, side])
                wait_for(slot_of(side, 3), rs_recv.at[group, side, 3])
            total, first, second = block_of(me), slot_of(0, 3), slot_of(1, 3)
            whole = (total[...].astype(F32) + first[...].astype(F32) + second[...].astype(F32)).astype(BF16)
            total[...] = whole
            final(whole.astype(F32))

    def hop_gu(lam, q, s):
        cols = span(q * fc, fc)

        def add_squares(g):
            squares_gu[...] += jnp.sum((g * g).reshape(-1, 8, fc), axis=0)

        hop(
            lam,
            q,
            s,
            q,
            lambda b: gu.at[lam, :, span(b * own_d, own_d), cols],
            lambda b, half: gu.at[lam, :, span(b * own_d + half * half_d, half_d), cols],
            lambda side, step: land_gu.at[q, side, step],
            lambda side, step, half: land_gu.at[q, side, step, :, pl.ds(half * half_d, half_d), :],
            add_squares,
        )

    def hop_gd(lam, h, s):
        def add_squares(g):
            squares_gd[...] += jnp.sum((g * g).reshape(-1, 8, own_f), axis=0)

        hop(
            lam,
            h,
            s,
            CHUNKS + h,
            lambda b: gd.at[lam, span(h * rows_d, rows_d), span(b * own_f, own_f)],
            lambda b, half: gd.at[lam, span(h * rows_d + half * half_r, half_r), span(b * own_f, own_f)],
            lambda side, step: land_gd.at[h, side, step],
            lambda side, step, half: land_gd.at[h, side, step, pl.ds(half * half_r, half_r), :],
            add_squares,
        )

    def tick(t):
        period = CHUNKS * PHASE

        def one(q, start, run):
            u = t - start
            s = lax.rem(jnp.maximum(u, 0), period)

            @pl.when((u >= 0) & (u < 2 * period) & (lax.rem(s, SPACING) == 0) & (s < 5 * SPACING))
            def _():
                run(lax.div(jnp.maximum(u, 0), period), q, lax.div(s, SPACING))

        def quarter(q, _):
            one(q, PHASE * (q + 1), hop_gu)
            return 0

        lax.fori_loop(0, CHUNKS, quarter, 0)

        def half(h, _):
            one(h, period + 1 + h, hop_gd)
            return 0

        lax.fori_loop(0, 2, half, 0)

    squares_gu[...] = jnp.zeros_like(squares_gu)
    squares_gd[...] = jnp.zeros_like(squares_gd)
    tm = tokens // 8
    tb = tokens // 4

    def norm_rows(i, src):
        rows = span(i * tm, tm)
        wide = src[rows, :].astype(F32)
        a[rows, :] = (wide * scale_of(wide)).astype(BF16)

    def transpose_rows(i, src, dst):
        rows = span(i * tm, tm)
        dst[:, rows] = src[rows, :].astype(F32).T.astype(BF16)

    for load in loads[:3]:
        load.wait()
    gather_round(0, 0, 0)
    gather_round(1, 0, 0)
    load_x.wait()
    lax.fori_loop(0, 8, lambda i, _: (norm_rows(i, xs), 0)[1], 0)
    gather_round(0, 0, 1)
    gather_round(1, 0, 1)
    load_dy.wait()
    lax.fori_loop(0, 8, lambda i, _: (transpose_rows(i, do, dot_do), 0)[1], 0)
    for r in (2, 3, 4):
        gather_round(0, 0, r)
        gather_round(1, 0, r)
    for load in loads[3:]:
        load.wait()
    gather_round(0, 1, 0)
    gather_round(1, 1, 0)
    gather_round(0, 0, 5)
    gathered(0, 0)
    gather_round(1, 0, 5)

    def hidden(i, _):
        rows = span(i * tm, tm)
        here = a[rows, :]
        for c in range(CHUNKS):
            cols = slice(c * fc, (c + 1) * fc)
            gate, up = dot(here, wgu[0, 0, :, cols]), dot(here, wgu[0, 1, :, cols])
            big[rows, cols] = (gate * sigmoid(gate) * up).astype(BF16)
        return 0

    lax.fori_loop(0, 2, hidden, 0)
    gather_round(0, 1, 1)
    gather_round(1, 1, 1)
    lax.fori_loop(2, 4, hidden, 0)
    gather_round(0, 1, 2)
    gather_round(1, 1, 2)
    lax.fori_loop(4, 6, hidden, 0)
    gather_round(0, 1, 3)
    gather_round(1, 1, 3)
    lax.fori_loop(6, 8, hidden, 0)
    gathered(1, 0)

    def down(i, _):
        rows = span(i * tm, tm)
        h = (xs[rows, :].astype(F32) + dot(big[rows, :], wd[0]).astype(BF16).astype(F32)).astype(BF16)
        h1[rows, :] = h
        wide = h.astype(F32)
        normed = wide * scale_of(wide)
        a[rows, :] = normed.astype(BF16)
        at[:, rows] = normed.astype(BF16).astype(F32).T.astype(BF16)
        return 0

    lax.fori_loop(0, 3, down, 0)
    gather_round(0, 1, 4)
    gather_round(1, 1, 4)
    lax.fori_loop(3, 8, down, 0)
    gather_round(0, 1, 5)
    gather_round(1, 1, 5)
    gathered(0, 1)
    gathered(1, 1)

    act_cols, gate_cols, up_cols = (slice(k * fc, (k + 1) * fc) for k in range(3))

    for lam in range(2):
        number = 1 - lam

        def quarter(c, _, lam=lam, number=number):
            cols = span(c * fc, fc)
            t0 = (lam * CHUNKS + c) * PHASE

            def rows_of(i, _):
                rows = span(i * tb, tb)
                here = a[rows, :]
                gate, up = dot(here, wgu[number, 0, :, cols]), dot(here, wgu[number, 1, :, cols])
                by_act = dot_t(do[rows, :], wd[number, cols, :]).astype(BF16).astype(F32)
                sig = sigmoid(gate)
                silu = gate * sig
                big[rows, act_cols] = (silu * up).astype(BF16)
                big[rows, up_cols] = (by_act * silu).astype(BF16)
                big[rows, gate_cols] = (by_act * up * (sig + silu * (1.0 - sig))).astype(BF16)
                tick(t0 + i)
                return 0

            lax.fori_loop(0, 4, rows_of, 0)
            gu[lam, 0, :, cols] = dot(at[...], big[:, gate_cols]).astype(BF16)
            tick(t0 + 4)
            gu[lam, 1, :, cols] = dot(at[...], big[:, up_cols]).astype(BF16)
            tick(t0 + 5)
            gd[lam, :, cols] = dot(dot_do[...], big[:, act_cols]).astype(BF16)
            tick(t0 + 6)
            if lam == 0:

                def by_input(i, _):
                    rows = span(i * tb, tb)
                    by_a = dot_t(big[rows, gate_cols], wgu[number, 0, :, cols]) + dot_t(big[rows, up_cols], wgu[number, 1, :, cols])

                    @pl.when(c == 0)
                    def _():
                        acc[rows, :] = by_a

                    @pl.when(c > 0)
                    def _():
                        acc[rows, :] += by_a

                    return 0

                lax.fori_loop(0, 4, by_input, 0)
            tick(t0 + 7)
            return 0

        lax.fori_loop(0, CHUNKS, quarter, 0)

        if lam == 0:

            def through_norm(i, _):
                rows = span(i * tm, tm)
                by_a = acc[rows, :].astype(BF16).astype(F32)
                wide = h1[rows, :].astype(F32)
                scale = scale_of(wide)
                inner = jnp.mean(by_a * wide, -1, keepdims=True)
                by_h = (by_a * scale - wide * (scale * scale * scale * inner)).astype(BF16).astype(F32)
                by_h = (do[rows, :].astype(F32) + by_h).astype(BF16)
                do[rows, :] = by_h
                dot_do[:, rows] = by_h.astype(F32).T.astype(BF16)
                wide = xs[rows, :].astype(F32)
                normed = (wide * scale_of(wide)).astype(BF16)
                a[rows, :] = normed
                at[:, rows] = normed.astype(F32).T.astype(BF16)
                return 0

            lax.fori_loop(0, 8, through_norm, 0)

    last = 2 * CHUNKS * PHASE + 4 * SPACING + 3
    lax.fori_loop(2 * CHUNKS * PHASE, last, lambda t, _: (tick(t), 0)[1], 0)

    outs = []
    for lam in range(2):
        outs.append(pltpu.make_async_copy(gu.at[lam, :, span(me * own_d, own_d), :], gu_out.at[1 - lam], out_sem.at[lam, 0]))
        outs.append(pltpu.make_async_copy(gd.at[lam, :, span(me * own_f, own_f)], gd_out.at[1 - lam], out_sem.at[lam, 1]))
    for out in outs:
        out.start()
    lanes = all_squares.shape[2]
    tile = sum(squares_gu[:, i * lanes : (i + 1) * lanes] for i in range(fc // lanes))
    tile = tile + sum(squares_gd[:, i * lanes : (i + 1) * lanes] for i in range(own_f // lanes))
    all_squares[me] = tile
    copies = [
        pltpu.make_async_remote_copy(
            src_ref=all_squares.at[me],
            dst_ref=all_squares.at[me],
            send_sem=sq_send.at[k - 1],
            recv_sem=sq_recv.at[k - 1],
            device_id={"dp": around(k)},
            device_id_type=MESH,
        )
        for k in range(1, n)
    ]
    for copy in copies:
        copy.start()
    for copy in copies:
        copy.wait()
    total = jnp.sum(all_squares[...])
    count = n * (gu_out.size + gd_out.size)
    factor_out[...] = jnp.minimum(1.0, 0.5 * lax.rsqrt(jnp.full(factor_out.shape, total, F32) / count + 1e-30))
    for kind in range(2):
        for number in range(2):
            await_eighths(kind, number, 56, ag_send.at[kind, number])
    for out in outs:
        out.wait()


def adamw(w, m, v, g):
    m = 0.9 * m + 0.1 * g
    v = 0.95 * v + 0.05 * g * g
    step = m * lax.rsqrt(v + 1e-8) + 0.1 * w
    return (w - 0.02 * step).astype(jnp.bfloat16), m, v


def solution(mesh):
    n, groups = mesh.shape["dp"], mesh.shape["rep"]
    across = math.isqrt(groups // 2)

    def step(x, dy, *arrays):
        weights, m, v = (arrays[i : i + 3] for i in (0, 3, 6))
        layers, own_d, ff = weights[0].shape
        own_f, d = weights[2].shape[1:]
        tokens = x.shape[1]
        fc = ff // CHUNKS
        lanes = min(128, own_f)
        anywhere = pl.BlockSpec(memory_space=pl.ANY)
        grads_gu, grads_gd, factor = pl.pallas_call(
            functools.partial(kernel, n, across),
            out_shape=(
                jax.ShapeDtypeStruct((layers, 2, own_d, ff), BF16),
                jax.ShapeDtypeStruct((layers, d, own_f), BF16),
                jax.ShapeDtypeStruct((8, lanes), F32),
            ),
            in_specs=[anywhere] * 5,
            out_specs=(anywhere, anywhere, pl.BlockSpec(memory_space=pltpu.VMEM)),
            scratch_shapes=[
                pltpu.VMEM((layers, 2, d, ff), BF16),
                pltpu.VMEM((layers, ff, d), BF16),
                pltpu.VMEM((layers, 2, d, ff), BF16),
                pltpu.VMEM((layers, d, ff), BF16),
                pltpu.VMEM((CHUNKS, 2, 4, 2, own_d, fc), BF16),
                pltpu.VMEM((2, 2, 4, d // 2, own_f), BF16),
                pltpu.VMEM((tokens, d), BF16),
                pltpu.VMEM((tokens, d), BF16),
                pltpu.VMEM((tokens, d), BF16),
                pltpu.VMEM((tokens, d), BF16),
                pltpu.VMEM((d, tokens), BF16),
                pltpu.VMEM((d, tokens), BF16),
                pltpu.VMEM((tokens, ff), BF16),
                pltpu.VMEM((tokens, d), F32),
                pltpu.VMEM((8, fc), F32),
                pltpu.VMEM((8, own_f), F32),
                pltpu.VMEM((n, 8, lanes), F32),
                pltpu.SemaphoreType.DMA((2, 4)),
                pltpu.SemaphoreType.DMA((2, 2)),
                pltpu.SemaphoreType.DMA((2, 2)),
                pltpu.SemaphoreType.DMA((2, 2, 4)),
                pltpu.SemaphoreType.DMA((2, 2, 4)),
                pltpu.SemaphoreType.DMA((2, 2)),
                pltpu.SemaphoreType.DMA((CHUNKS + 2, 2)),
                pltpu.SemaphoreType.DMA((CHUNKS + 2, 2, 4)),
                pltpu.SemaphoreType.DMA((n - 1,)),
                pltpu.SemaphoreType.DMA((n - 1,)),
            ],
            compiler_params=pltpu.CompilerParams(collective_id=0, has_side_effects=True, vmem_limit_bytes=67043328),
            name="train_step",
        )(x, dy, *weights)
        factor = factor[0, 0]
        gradients = [grads_gu[:, 0], grads_gu[:, 1], jnp.swapaxes(grads_gd, 1, 2)]
        new = [adamw(w.astype(F32), m, v, g.astype(F32) * factor) for w, m, v, g in zip(weights, m, v, gradients, strict=True)]
        return tuple(one[which] for which in range(3) for one in new)

    states, cut = P(("rep", "dp"), None, None), P(None, "dp", None)
    return jax.shard_map(
        step,
        mesh=mesh,
        in_specs=(states, states) + (cut,) * 9,
        out_specs=(P("rep", "dp", None),) * 9,
        check_vma=False,
    )
```

```python
import functools
import math

import jax
import jax.numpy as jnp
from jax import lax
from jax.experimental import pallas as pl
from jax.experimental.pallas import tpu as pltpu
from jax.sharding import PartitionSpec as P

MESH = pl.DeviceIdType.MESH
F32, BF16 = jnp.float32, jnp.bfloat16
CHUNKS = 4
SPACING = 5
PHASE = 8
START = 5
PERIOD = (CHUNKS + 1) * PHASE


def dot(a, b):
    return jnp.dot(a, b, preferred_element_type=F32)


def dot_t(a, b):
    return lax.dot_general(a, b, (((1,), (1,)), ((), ())), preferred_element_type=F32)


def sigmoid(x):
    return 0.5 * jnp.tanh(0.5 * x) + 0.5


def scale_of(wide):
    return lax.rsqrt(jnp.mean(wide * wide, -1, keepdims=True) + 1e-6)


def span(start, size):
    return pl.ds(pl.multiple_of(start, size), size)


def kernel(
    n,
    across,
    x_in,
    dy_in,
    wg_in,
    wu_in,
    wd_in,
    g_out,
    u_out,
    d_out,
    factor_out,
    wgu,
    wd,
    gu,
    gd,
    land_gu,
    land_gd,
    xs,
    do,
    h1,
    a,
    at,
    dot_do,
    act,
    by_gu,
    d_own,
    squares_gu,
    squares_gd,
    all_squares,
    load_sem,
    out_sem,
    ag_send,
    ag_z,
    ag_pair,
    ag_core,
    rs_send,
    rs_recv,
    sq_send,
    sq_recv,
):
    tokens, d = xs.shape
    ff = wgu.shape[3]
    own_d, own_f = d // n, ff // n
    fc = ff // CHUNKS
    me, rep = lax.axis_index("dp"), lax.axis_index("rep")
    core, y_bit, x_bit = rep % 2, (rep // 2) % 2, (rep // (2 * across)) % 2
    parity = (x_bit + y_bit) % 2

    def around(k):
        return lax.rem(me + (k + n), n)

    right, left = {"dp": around(1)}, {"dp": around(-1)}
    other_core = {"rep": rep + 1 - 2 * core}
    other_y = {"rep": rep + 2 - 4 * y_bit}
    other_x = {"rep": rep + 2 * across * (1 - 2 * x_bit)}

    barrier = pltpu.get_barrier_semaphore()
    partners = [{"dp": around(k)} for k in range(1, n)] + [other_core, other_y, other_x]
    for partner in partners:
        pl.semaphore_signal(barrier, inc=1, device_id=partner, device_id_type=MESH)

    loads = []
    for number in range(2):
        loads.append(pltpu.make_async_copy(wg_in.at[number], wgu.at[number, 0, span(me * own_d, own_d), :], load_sem.at[number, 0]))
        loads.append(pltpu.make_async_copy(wu_in.at[number], wgu.at[number, 1, span(me * own_d, own_d), :], load_sem.at[number, 1]))
        loads.append(pltpu.make_async_copy(wd_in.at[number], wd.at[number, span(me * own_f, own_f), :], load_sem.at[number, 2]))
    load_x = pltpu.make_async_copy(x_in.at[0], xs, load_sem.at[0, 3])
    load_dy = pltpu.make_async_copy(dy_in.at[0], do, load_sem.at[1, 3])
    for load in loads[:3] + [load_x] + loads[3:] + [load_dy]:
        load.start()
    pl.semaphore_wait(barrier, len(partners))

    eighth_f, eighth_r = ff // 8, own_f // 8
    mine = 4 * core + 2 * parity
    theirs = 4 * core + 2 * (1 - parity)

    def part(kind, number, shard, eighth, count):
        if kind < 2:
            return wgu.at[number, kind, span(shard * own_d, own_d), pl.ds(pl.multiple_of(eighth * eighth_f, eighth_f), count * eighth_f)]
        return wd.at[number, pl.ds(pl.multiple_of(shard * own_f + eighth * eighth_r, eighth_r), count * eighth_r), :]

    def bytes_of(kind, number, eighths):
        if kind < 2:
            return wgu.at[number, kind, pl.ds(0, eighths * own_d // 8), :]
        return wd.at[number, pl.ds(0, eighths * eighth_r), :]

    def await_eighths(kind, number, eighths, sem):
        ref = bytes_of(kind, number, eighths)
        pltpu.make_async_copy(ref, ref, sem).wait()

    def push(kind, number, shard, eighth, count, recv_sem, device):
        ref = part(kind, number, shard, eighth, count)
        pltpu.make_async_remote_copy(
            src_ref=ref, dst_ref=ref, send_sem=ag_send.at[kind, number], recv_sem=recv_sem, device_id=device, device_id_type=MESH
        ).start()

    def gather_round(kind, number, r):
        core_sem = ag_core.at[kind, number]
        if r >= 1 and r <= 4:
            await_eighths(kind, number, 4 if r <= 3 else 2, ag_z.at[kind, number, r - 1])
        if r <= 2:
            push(kind, number, around(-r), mine, 2, ag_z.at[kind, number, r], right)
            push(kind, number, around(r), mine, 2, ag_z.at[kind, number, r], left)
        elif r == 3:
            push(kind, number, around(-r), mine, 1, ag_z.at[kind, number, r], right)
            push(kind, number, around(r), mine + 1, 1, ag_z.at[kind, number, r], left)
        if r >= 1 and r <= 4:
            for shard in (around(-r), around(r)) if r <= 3 else (around(r),):
                push(kind, number, shard, mine, 1, ag_pair.at[kind, number, r - 1], other_y)
                push(kind, number, shard, mine + 1, 1, ag_pair.at[kind, number, r - 1], other_x)
                push(kind, number, shard, mine, 2, core_sem, other_core)
        if r >= 2:
            s = r - 1
            await_eighths(kind, number, 4 if s <= 3 else 2, ag_pair.at[kind, number, s - 1])
            for shard in (around(-s), around(s)) if s <= 3 else (around(s),):
                push(kind, number, shard, theirs, 2, core_sem, other_core)

    def gathered(kind, number):
        await_eighths(kind, number, 28, ag_core.at[kind, number])

    half_d = own_d // 2
    rows_d = d // 2
    half_r = rows_d // 2
    sides = ((right, 1), (left, -1))

    def wait_for(ref, sem):
        pltpu.make_async_copy(ref, ref, sem).wait()

    def hop(lam, q, s, group, block_of, half_of, slot_of, slot_half_of, final):
        for side, (device, sign) in enumerate(sides):
            send, recv = rs_send.at[group, side], rs_recv.at[group, side]
            block = lax.rem(me + sign * (4 - s) + n, n)

            def go(src, dst, step, send=send, recv=recv, device=device):
                pltpu.make_async_remote_copy(
                    src_ref=src, dst_ref=dst, send_sem=send, recv_sem=recv.at[step], device_id=device, device_id_type=MESH
                ).start()

            @pl.when(s == 0)
            def _(side=side, block=block, go=go):
                go(half_of(block, side), slot_half_of(side), 0)

            @pl.when(s == 1)
            def _(side=side, block=block, go=go, send=send, recv=recv):
                wait_for(slot_half_of(side), send)
                wait_for(slot_half_of(side), recv.at[0])
                total, arrived = half_of(block, side), slot_half_of(side)
                total[...] = (total[...].astype(F32) + arrived[...].astype(F32)).astype(BF16)
                go(block_of(block), slot_of(side, 1), 1)

            @pl.when((s == 2) | (s == 3))
            def _(side=side, block=block, go=go, send=send, recv=recv):
                wait_for(slot_of(side, s - 1), send)
                wait_for(slot_of(side, s - 1), recv.at[s - 1])
                total, arrived = block_of(block), slot_of(side, s - 1)
                total[...] = (total[...].astype(F32) + arrived[...].astype(F32)).astype(BF16)
                go(block_of(block), slot_of(side, s), s)

        @pl.when(s == 4)
        def _():
            for side in range(2):
                wait_for(slot_of(side, 3), rs_send.at[group, side])
                wait_for(slot_of(side, 3), rs_recv.at[group, side, 3])
            total, first, second = block_of(me), slot_of(0, 3), slot_of(1, 3)
            whole = (total[...].astype(F32) + first[...].astype(F32) + second[...].astype(F32)).astype(BF16)
            final(total, whole)

    def hop_gu(lam, q, s):
        cols = span(q * fc, fc)

        def finish(total, whole):
            total[...] = whole
            g = whole.astype(F32)
            squares_gu[...] += jnp.sum((g * g).reshape(-1, 8, fc), axis=0)

        hop(
            lam,
            q,
            s,
            q,
            lambda b: gu.at[lam, :, span(b * own_d, own_d), cols],
            lambda b, half: gu.at[lam, :, span(b * own_d + half * half_d, half_d), cols],
            lambda side, step: land_gu.at[q, side, :, pl.ds(pl.multiple_of((2 * step - 1) * half_d, half_d), own_d), :],
            lambda side: land_gu.at[q, side, :, pl.ds(0, half_d), :],
            finish,
        )

    def hop_gd(lam, h, s):
        def finish(total, whole):
            g = whole.astype(F32)
            d_own[lam, :, span(h * rows_d, rows_d)] = g.T.astype(BF16)
            squares_gd[...] += jnp.sum((g * g).reshape(-1, 8, own_f), axis=0)

        hop(
            lam,
            h,
            s,
            CHUNKS + h,
            lambda b: gd.at[lam, span(h * rows_d, rows_d), span(b * own_f, own_f)],
            lambda b, half: gd.at[lam, span(h * rows_d + half * half_r, half_r), span(b * own_f, own_f)],
            lambda side, step: land_gd.at[h, side, pl.ds(pl.multiple_of((2 * step - 1) * half_r, half_r), rows_d), :],
            lambda side: land_gd.at[h, side, pl.ds(0, half_r), :],
            finish,
        )

    def tick(t):
        def one(q, start, run):
            u = t - start
            s = lax.rem(jnp.maximum(u, 0), PERIOD)

            @pl.when((u >= 0) & (u < 2 * PERIOD) & (lax.rem(s, SPACING) == 0) & (s < 5 * SPACING))
            def _():
                run(lax.div(jnp.maximum(u, 0), PERIOD), q, lax.div(s, SPACING))

        def quarter(q, _):
            one(q, PHASE * q + START, hop_gu)
            return 0

        lax.fori_loop(0, CHUNKS, quarter, 0)

        def half(h, _):
            one(h, PHASE * CHUNKS + h, hop_gd)
            return 0

        lax.fori_loop(0, 2, half, 0)

    squares_gu[...] = jnp.zeros_like(squares_gu)
    squares_gd[...] = jnp.zeros_like(squares_gd)
    tm = tokens // 8
    tb = tokens // 4

    def norm_rows(i, src):
        rows = span(i * tm, tm)
        wide = src[rows, :].astype(F32)
        a[rows, :] = (wide * scale_of(wide)).astype(BF16)

    def transpose_rows(i, src, dst):
        rows = span(i * tm, tm)
        dst[:, rows] = src[rows, :].astype(F32).T.astype(BF16)

    def rounds(number, r, kinds=(0, 1, 2)):
        for kind in kinds:
            gather_round(kind, number, r)

    def loop(first, end, body):
        lax.fori_loop(first, end, lambda i, _: (body(i), 0)[1], 0)

    for load in loads[:3]:
        load.wait()
    rounds(0, 0)
    load_x.wait()
    loop(0, 8, lambda i: norm_rows(i, xs))
    rounds(0, 1)
    load_dy.wait()
    loop(0, 3, lambda i: transpose_rows(i, do, dot_do))
    rounds(0, 2)
    loop(3, 6, lambda i: transpose_rows(i, do, dot_do))
    rounds(0, 3)
    for load in loads[3:]:
        load.wait()
    rounds(1, 0)
    loop(6, 8, lambda i: transpose_rows(i, do, dot_do))
    rounds(0, 4)
    rounds(0, 5)
    gathered(0, 0)
    gathered(1, 0)

    later = [(kind, r) for r in range(1, 6) for kind in range(3)]
    slots = [4 * (r - 1) + kind + 1 for kind, r in later]

    def between(i, first, end):
        for slot, (kind, r) in zip(slots, later, strict=True):
            if first <= slot < end:

                @pl.when(i == slot)
                def _(kind=kind, r=r):
                    gather_round(kind, 1, r)

    def hidden(i):
        rows = span(lax.div(i, 2) * tm, tm)
        here = a[rows, :]
        for c in range(CHUNKS // 2):
            cols = span((lax.rem(i, 2) * (CHUNKS // 2) + c) * fc, fc)
            gate, up = dot(here, wgu[0, 0, :, cols]), dot(here, wgu[0, 1, :, cols])
            by_gu[0, rows, cols] = (gate * sigmoid(gate) * up).astype(BF16)
        between(i, 0, 16)

    loop(0, 16, hidden)
    gathered(2, 0)

    def down(i):
        rows = span(i * tm, tm)
        h = (xs[rows, :].astype(F32) + dot(by_gu[0, rows, :], wd[0]).astype(BF16).astype(F32)).astype(BF16)
        h1[rows, :] = h
        wide = h.astype(F32)
        normed = (wide * scale_of(wide)).astype(BF16)
        a[rows, :] = normed
        at[:, rows] = normed.astype(F32).T.astype(BF16)
        between(i + 16, 16, 24)

    loop(0, 8, down)
    for kind in range(3):
        gathered(kind, 1)

    for lam in range(2):
        number = 1 - lam

        def quarter(c, lam=lam, number=number):
            cols = span(c * fc, fc)
            t0 = lam * PERIOD + c * PHASE

            def rows_of(i):
                rows = span(i * tb, tb)
                here = a[rows, :]
                gate, up = dot(here, wgu[number, 0, :, cols]), dot(here, wgu[number, 1, :, cols])
                by_act = dot_t(do[rows, :], wd[number, cols, :]).astype(BF16).astype(F32)
                sig = sigmoid(gate)
                silu = gate * sig
                act[rows, :] = (silu * up).astype(BF16)
                by_gu[1, rows, cols] = (by_act * silu).astype(BF16)
                by_gu[0, rows, cols] = (by_act * up * (sig + silu * (1.0 - sig))).astype(BF16)
                tick(t0 + i)

            loop(0, 4, rows_of)
            gu[lam, 0, :, cols] = dot(at[...], by_gu[0, :, cols]).astype(BF16)
            tick(t0 + 4)
            gu[lam, 1, :, cols] = dot(at[...], by_gu[1, :, cols]).astype(BF16)
            tick(t0 + 5)

            def by_down(i):
                rows = span(i * rows_d, rows_d)
                gd[lam, rows, cols] = dot(dot_do[rows, :], act[...]).astype(BF16)
                tick(t0 + 6 + i)

            loop(0, 2, by_down)

        loop(0, CHUNKS, quarter)

        if lam == 0:
            t0 = CHUNKS * PHASE

            def by_input(i, number=number, t0=t0):
                rows = span(i * tm, tm)
                by_a = dot_t(by_gu[0, rows, :], wgu[number, 0]) + dot_t(by_gu[1, rows, :], wgu[number, 1])
                by_a = by_a.astype(BF16).astype(F32)
                wide = h1[rows, :].astype(F32)
                scale = scale_of(wide)
                inner = jnp.mean(by_a * wide, -1, keepdims=True)
                by_h = (by_a * scale - wide * (scale * scale * scale * inner)).astype(BF16).astype(F32)
                by_h = (do[rows, :].astype(F32) + by_h).astype(BF16)
                do[rows, :] = by_h
                dot_do[:, rows] = by_h.astype(F32).T.astype(BF16)
                wide = xs[rows, :].astype(F32)
                normed = (wide * scale_of(wide)).astype(BF16)
                a[rows, :] = normed
                at[:, rows] = normed.astype(F32).T.astype(BF16)
                tick(t0 + i)

            loop(0, 8, by_input)

    loop(PERIOD + CHUNKS * PHASE, PERIOD + CHUNKS * PHASE + 4 * SPACING + 2, tick)

    outs = []
    for lam in range(2):
        for kind, out in enumerate((g_out, u_out)):
            own = gu.at[lam, kind, span(me * own_d, own_d), :]
            outs.append(pltpu.make_async_copy(own, out.at[1 - lam], out_sem.at[lam, kind]))
        outs.append(pltpu.make_async_copy(d_own.at[lam], d_out.at[1 - lam], out_sem.at[lam, 2]))
    for out in outs:
        out.start()
    lanes = all_squares.shape[2]
    tile = sum(squares_gu[:, i * lanes : (i + 1) * lanes] for i in range(fc // lanes))
    tile = tile + sum(squares_gd[:, i * lanes : (i + 1) * lanes] for i in range(own_f // lanes))
    all_squares[me] = tile
    copies = [
        pltpu.make_async_remote_copy(
            src_ref=all_squares.at[me],
            dst_ref=all_squares.at[me],
            send_sem=sq_send.at[k - 1],
            recv_sem=sq_recv.at[k - 1],
            device_id={"dp": around(k)},
            device_id_type=MESH,
        )
        for k in range(1, n)
    ]
    for copy in copies:
        copy.start()
    for copy in copies:
        copy.wait()
    total = jnp.sum(all_squares[...])
    count = n * (g_out.size + u_out.size + d_out.size)
    factor_out[...] = jnp.minimum(1.0, 0.5 * lax.rsqrt(jnp.full(factor_out.shape, total, F32) / count + 1e-30))
    for kind in range(3):
        for number in range(2):
            await_eighths(kind, number, 56, ag_send.at[kind, number])
    for out in outs:
        out.wait()


def adamw(w, m, v, g):
    m = 0.9 * m + 0.1 * g
    v = 0.95 * v + 0.05 * g * g
    step = m * lax.rsqrt(v + 1e-8) + 0.1 * w
    return (w - 0.02 * step).astype(jnp.bfloat16), m, v


def update(factor, *refs):
    ins, outs = refs[:12], refs[12:]
    for i in range(3):
        w, m, v, g = (ins[3 * k + i] for k in range(4))
        new = adamw(w[...].astype(F32), m[...], v[...], g[...].astype(F32) * factor[0, 0])
        for k in range(3):
            outs[3 * k + i][...] = new[k]


def solution(mesh):
    n, groups = mesh.shape["dp"], mesh.shape["rep"]
    across = math.isqrt(groups // 2)

    def step(x, dy, *arrays):
        weights, m, v = (arrays[i : i + 3] for i in (0, 3, 6))
        layers, own_d, ff = weights[0].shape
        own_f, d = weights[2].shape[1:]
        tokens = x.shape[1]
        fc = ff // CHUNKS
        lanes = min(128, own_f)
        anywhere = pl.BlockSpec(memory_space=pl.ANY)
        *gradients, factor = pl.pallas_call(
            functools.partial(kernel, n, across),
            out_shape=(
                jax.ShapeDtypeStruct((layers, own_d, ff), BF16),
                jax.ShapeDtypeStruct((layers, own_d, ff), BF16),
                jax.ShapeDtypeStruct((layers, own_f, d), BF16),
                jax.ShapeDtypeStruct((8, lanes), F32),
            ),
            in_specs=[anywhere] * 5,
            out_specs=(anywhere, anywhere, anywhere, pl.BlockSpec(memory_space=pltpu.VMEM)),
            scratch_shapes=[
                pltpu.VMEM((layers, 2, d, ff), BF16),
                pltpu.VMEM((layers, ff, d), BF16),
                pltpu.VMEM((layers, 2, d, ff), BF16),
                pltpu.VMEM((layers, d, ff), BF16),
                pltpu.VMEM((CHUNKS, 2, 2, 7 * own_d // 2, fc), BF16),
                pltpu.VMEM((2, 2, 7 * d // 4, own_f), BF16),
                pltpu.VMEM((tokens, d), BF16),
                pltpu.VMEM((tokens, d), BF16),
                pltpu.VMEM((tokens, d), BF16),
                pltpu.VMEM((tokens, d), BF16),
                pltpu.VMEM((d, tokens), BF16),
                pltpu.VMEM((d, tokens), BF16),
                pltpu.VMEM((tokens, fc), BF16),
                pltpu.VMEM((2, tokens, ff), BF16),
                pltpu.VMEM((layers, own_f, d), BF16),
                pltpu.VMEM((8, fc), F32),
                pltpu.VMEM((8, own_f), F32),
                pltpu.VMEM((n, 8, lanes), F32),
                pltpu.SemaphoreType.DMA((2, 4)),
                pltpu.SemaphoreType.DMA((2, 3)),
                pltpu.SemaphoreType.DMA((3, 2)),
                pltpu.SemaphoreType.DMA((3, 2, 4)),
                pltpu.SemaphoreType.DMA((3, 2, 4)),
                pltpu.SemaphoreType.DMA((3, 2)),
                pltpu.SemaphoreType.DMA((CHUNKS + 2, 2)),
                pltpu.SemaphoreType.DMA((CHUNKS + 2, 2, 4)),
                pltpu.SemaphoreType.DMA((n - 1,)),
                pltpu.SemaphoreType.DMA((n - 1,)),
            ],
            compiler_params=pltpu.CompilerParams(collective_id=0, has_side_effects=True, vmem_limit_bytes=67043328),
            name="train_step",
        )(x, dy, *weights)
        pieces = 4

        def blocks(arrays):
            return tuple(
                pl.BlockSpec((1, one.shape[1] // pieces, one.shape[2]), lambda layer, piece: (layer, piece, 0)) for one in arrays
            )

        shapes = [jax.ShapeDtypeStruct(one.shape, kind) for kind in (BF16, F32, F32) for one in weights]
        inputs = (*weights, *m, *v, *gradients)
        return pl.pallas_call(
            update,
            grid=(layers, pieces),
            out_shape=tuple(shapes),
            in_specs=[pl.BlockSpec(memory_space=pltpu.SMEM), *blocks(inputs)],
            out_specs=blocks(shapes),
            name="adamw",
        )(factor, *inputs)

    states, cut = P(("rep", "dp"), None, None), P(None, "dp", None)
    return jax.shard_map(
        step,
        mesh=mesh,
        in_specs=(states, states) + (cut,) * 9,
        out_specs=(P("rep", "dp", None),) * 9,
        check_vma=False,
    )
```

```python
import functools
import math

import jax
import jax.numpy as jnp
from jax import lax
from jax.experimental import pallas as pl
from jax.experimental.pallas import tpu as pltpu
from jax.sharding import PartitionSpec as P

MESH = pl.DeviceIdType.MESH
F32, BF16 = jnp.float32, jnp.bfloat16
CHUNKS = 4
SPACING = 5
PHASE = 8
START = 5
PERIOD = (CHUNKS + 1) * PHASE


def dot(a, b):
    return jnp.dot(a, b, preferred_element_type=F32)


def dot_t(a, b):
    return lax.dot_general(a, b, (((1,), (1,)), ((), ())), preferred_element_type=F32)


def sigmoid(x):
    return 0.5 * jnp.tanh(0.5 * x) + 0.5


def scale_of(wide):
    return lax.rsqrt(jnp.mean(wide * wide, -1, keepdims=True) + 1e-6)


def span(start, size):
    return pl.ds(pl.multiple_of(start, size), size)


def kernel(
    n,
    across,
    x_in,
    dy_in,
    wg_in,
    wu_in,
    wd_in,
    g_out,
    u_out,
    d_out,
    factor_out,
    wgu,
    wd,
    gu,
    gd,
    land_gu,
    land_gd,
    xs,
    do,
    h1,
    a,
    at,
    dot_do,
    act,
    by_gu,
    d_own,
    squares_gu,
    squares_gd,
    all_squares,
    load_sem,
    out_sem,
    ag_send,
    ag_z,
    ag_pair,
    ag_core,
    rs_send,
    rs_recv,
    sq_send,
    sq_recv,
):
    tokens, d = xs.shape
    ff = wgu.shape[3]
    own_d, own_f = d // n, ff // n
    fc = ff // CHUNKS
    me, rep = lax.axis_index("dp"), lax.axis_index("rep")
    core, y_bit, x_bit = rep % 2, (rep // 2) % 2, (rep // (2 * across)) % 2
    parity = (x_bit + y_bit) % 2

    def around(k):
        return lax.rem(me + (k + n), n)

    right, left = {"dp": around(1)}, {"dp": around(-1)}
    other_core = {"rep": rep + 1 - 2 * core}
    other_y = {"rep": rep + 2 - 4 * y_bit}
    other_x = {"rep": rep + 2 * across * (1 - 2 * x_bit)}

    barrier = pltpu.get_barrier_semaphore()
    partners = [{"dp": around(k)} for k in range(1, n)] + [other_core, other_y, other_x]
    for partner in partners:
        pl.semaphore_signal(barrier, inc=1, device_id=partner, device_id_type=MESH)

    loads = []
    for number in range(2):
        loads.append(pltpu.make_async_copy(wg_in.at[number], wgu.at[number, 0, span(me * own_d, own_d), :], load_sem.at[number, 0]))
        loads.append(pltpu.make_async_copy(wu_in.at[number], wgu.at[number, 1, span(me * own_d, own_d), :], load_sem.at[number, 1]))
        loads.append(pltpu.make_async_copy(wd_in.at[number], wd.at[number, span(me * own_f, own_f), :], load_sem.at[number, 2]))
    load_x = pltpu.make_async_copy(x_in.at[0], xs, load_sem.at[0, 3])
    load_dy = pltpu.make_async_copy(dy_in.at[0], do, load_sem.at[1, 3])
    for load in loads[:3] + [load_x] + loads[3:] + [load_dy]:
        load.start()
    pl.semaphore_wait(barrier, len(partners))

    eighth_f, eighth_r = ff // 16, own_f // 8
    mine = 4 * core + 2 * parity
    theirs = 4 * core + 2 * (1 - parity)

    def part(kind, number, shard, eighth, count):
        if kind < 4:
            column = pl.multiple_of((kind // 2 * 8 + eighth) * eighth_f, eighth_f)
            return wgu.at[number, kind % 2, span(shard * own_d, own_d), pl.ds(column, count * eighth_f)]
        return wd.at[number, pl.ds(pl.multiple_of(shard * own_f + eighth * eighth_r, eighth_r), count * eighth_r), :]

    def bytes_of(kind, number, eighths):
        if kind < 4:
            return wgu.at[number, kind % 2, pl.ds(0, eighths * own_d // 8), pl.ds(0, ff // 2)]
        return wd.at[number, pl.ds(0, eighths * eighth_r), :]

    def await_eighths(kind, number, eighths, sem):
        ref = bytes_of(kind, number, eighths)
        pltpu.make_async_copy(ref, ref, sem).wait()

    def push(kind, number, shard, eighth, count, recv_sem, device):
        ref = part(kind, number, shard, eighth, count)
        pltpu.make_async_remote_copy(
            src_ref=ref, dst_ref=ref, send_sem=ag_send.at[kind, number], recv_sem=recv_sem, device_id=device, device_id_type=MESH
        ).start()

    def gather_round(kind, number, r):
        core_sem = ag_core.at[kind, number]
        if r >= 1 and r <= 4:
            await_eighths(kind, number, 4 if r <= 3 else 2, ag_z.at[kind, number, r - 1])
        if r <= 2:
            push(kind, number, around(-r), mine, 2, ag_z.at[kind, number, r], right)
            push(kind, number, around(r), mine, 2, ag_z.at[kind, number, r], left)
        elif r == 3:
            push(kind, number, around(-r), mine, 1, ag_z.at[kind, number, r], right)
            push(kind, number, around(r), mine + 1, 1, ag_z.at[kind, number, r], left)
        if r >= 1 and r <= 4:
            for shard in (around(-r), around(r)) if r <= 3 else (around(r),):
                push(kind, number, shard, mine, 1, ag_pair.at[kind, number, r - 1], other_y)
                push(kind, number, shard, mine + 1, 1, ag_pair.at[kind, number, r - 1], other_x)
                push(kind, number, shard, mine, 2, core_sem, other_core)
        if r >= 2:
            s = r - 1
            await_eighths(kind, number, 4 if s <= 3 else 2, ag_pair.at[kind, number, s - 1])
            for shard in (around(-s), around(s)) if s <= 3 else (around(s),):
                push(kind, number, shard, theirs, 2, core_sem, other_core)

    def gathered(kind, number):
        await_eighths(kind, number, 28, ag_core.at[kind, number])

    half_d = own_d // 2
    rows_d = d // 2
    half_r = rows_d // 2
    sides = ((right, 1), (left, -1))

    def wait_for(ref, sem):
        pltpu.make_async_copy(ref, ref, sem).wait()

    def hop(lam, q, s, group, block_of, half_of, slot_of, slot_half_of, final):
        for side, (device, sign) in enumerate(sides):
            send, recv = rs_send.at[group, side], rs_recv.at[group, side]
            block = lax.rem(me + sign * (4 - s) + n, n)

            def go(src, dst, step, send=send, recv=recv, device=device):
                pltpu.make_async_remote_copy(
                    src_ref=src, dst_ref=dst, send_sem=send, recv_sem=recv.at[step], device_id=device, device_id_type=MESH
                ).start()

            @pl.when(s == 0)
            def _(side=side, block=block, go=go):
                go(half_of(block, side), slot_half_of(side), 0)

            @pl.when(s == 1)
            def _(side=side, block=block, go=go, send=send, recv=recv):
                wait_for(slot_half_of(side), send)
                wait_for(slot_half_of(side), recv.at[0])
                total, arrived = half_of(block, side), slot_half_of(side)
                total[...] = (total[...].astype(F32) + arrived[...].astype(F32)).astype(BF16)
                go(block_of(block), slot_of(side, 1), 1)

            @pl.when((s == 2) | (s == 3))
            def _(side=side, block=block, go=go, send=send, recv=recv):
                wait_for(slot_of(side, s - 1), send)
                wait_for(slot_of(side, s - 1), recv.at[s - 1])
                total, arrived = block_of(block), slot_of(side, s - 1)
                total[...] = (total[...].astype(F32) + arrived[...].astype(F32)).astype(BF16)
                go(block_of(block), slot_of(side, s), s)

        @pl.when(s == 4)
        def _():
            for side in range(2):
                wait_for(slot_of(side, 3), rs_send.at[group, side])
                wait_for(slot_of(side, 3), rs_recv.at[group, side, 3])
            total, first, second = block_of(me), slot_of(0, 3), slot_of(1, 3)
            whole = (total[...].astype(F32) + first[...].astype(F32) + second[...].astype(F32)).astype(BF16)
            final(total, whole)

    def hop_gu(lam, q, s):
        cols = span(q * fc, fc)

        def finish(total, whole):
            total[...] = whole
            g = whole.astype(F32)
            squares_gu[...] += jnp.sum((g * g).reshape(-1, 8, fc), axis=0)

        hop(
            lam,
            q,
            s,
            q,
            lambda b: gu.at[lam, :, span(b * own_d, own_d), cols],
            lambda b, half: gu.at[lam, :, span(b * own_d + half * half_d, half_d), cols],
            lambda side, step: land_gu.at[q, side, :, pl.ds(pl.multiple_of((2 * step - 1) * half_d, half_d), own_d), :],
            lambda side: land_gu.at[q, side, :, pl.ds(0, half_d), :],
            finish,
        )

    def hop_gd(lam, h, s):
        def finish(total, whole):
            g = whole.astype(F32)
            d_own[lam, :, span(h * rows_d, rows_d)] = g.T.astype(BF16)
            squares_gd[...] += jnp.sum((g * g).reshape(-1, 8, own_f), axis=0)

        hop(
            lam,
            h,
            s,
            CHUNKS + h,
            lambda b: gd.at[lam, span(h * rows_d, rows_d), span(b * own_f, own_f)],
            lambda b, half: gd.at[lam, span(h * rows_d + half * half_r, half_r), span(b * own_f, own_f)],
            lambda side, step: land_gd.at[h, side, pl.ds(pl.multiple_of((2 * step - 1) * half_r, half_r), rows_d), :],
            lambda side: land_gd.at[h, side, pl.ds(0, half_r), :],
            finish,
        )

    def tick(t):
        def one(q, start, run):
            u = t - start
            s = lax.rem(jnp.maximum(u, 0), PERIOD)

            @pl.when((u >= 0) & (u < 2 * PERIOD) & (lax.rem(s, SPACING) == 0) & (s < 5 * SPACING))
            def _():
                run(lax.div(jnp.maximum(u, 0), PERIOD), q, lax.div(s, SPACING))

        def quarter(q, _):
            one(q, PHASE * q + START, hop_gu)
            return 0

        lax.fori_loop(0, CHUNKS, quarter, 0)

        def half(h, _):
            one(h, PHASE * CHUNKS + h, hop_gd)
            return 0

        lax.fori_loop(0, 2, half, 0)

    squares_gu[...] = jnp.zeros_like(squares_gu)
    squares_gd[...] = jnp.zeros_like(squares_gd)
    tm = tokens // 8

    def norm_rows(i, src):
        rows = span(i * tm, tm)
        wide = src[rows, :].astype(F32)
        a[rows, :] = (wide * scale_of(wide)).astype(BF16)

    def transpose_rows(i, src, dst):
        rows = span(i * tm, tm)
        dst[:, rows] = src[rows, :].astype(F32).T.astype(BF16)

    def loop(first, end, body):
        lax.fori_loop(first, end, lambda i, _: (body(i), 0)[1], 0)

    first, second, third = "1024..3.1..0.2.56310243106298.1036415029837", "....5.46..239.5.476...594..6..5.9.....9..7", "..8..7...8..7.8.....78."
    early, woven, taken, slot = [], [], [0] * 10, -1
    for place, mark in enumerate(first + second + third):
        if mark == ".":
            slot += place >= len(first)
            early += [None] * (place < len(first))
        else:
            number, kind = divmod(int(mark), 5)
            one = (number, kind, taken[int(mark)])
            taken[int(mark)] += 1
            (woven if place >= len(first) else early).append((slot, *one) if place >= len(first) else one)

    def between(i, *ranges):
        for slot, number, kind, r in woven:
            if any(slot in one for one in ranges):

                @pl.when(i == slot)
                def _(number=number, kind=kind, r=r):
                    gather_round(kind, number, r)

    for load in loads[:3]:
        load.wait()
    waiting = [
        lambda: (load_x.wait(), loop(0, 4, lambda i: norm_rows(i, xs))),
        lambda: loop(4, 8, lambda i: norm_rows(i, xs)),
        lambda: [load.wait() for load in loads[3:]],
        lambda: (load_dy.wait(), loop(0, 2, lambda i: transpose_rows(i, do, dot_do))),
        lambda: loop(2, 4, lambda i: transpose_rows(i, do, dot_do)),
        lambda: loop(4, 6, lambda i: transpose_rows(i, do, dot_do)),
        lambda: loop(6, 8, lambda i: transpose_rows(i, do, dot_do)),
    ]
    for one in early:
        if one:
            number, kind, r = one
            gather_round(kind, number, r)
        else:
            waiting.pop(0)() if waiting else None
    for kind in range(2):
        gathered(kind, 0)

    def hidden(i):
        rows = span(lax.rem(i, 8) * tm, tm)
        here = a[rows, :]
        parts = [span((lax.div(i, 8) * (CHUNKS // 2) + c) * fc, fc) for c in range(CHUNKS // 2)]
        products = [(dot(here, wgu[0, 0, :, cols]), dot(here, wgu[0, 1, :, cols])) for cols in parts]
        for cols, (gate, up) in zip(parts, products, strict=True):
            by_gu[0, rows, cols] = (gate * sigmoid(gate) * up).astype(BF16)
        between(i, range(16))

    loop(0, 8, hidden)
    for kind in (2, 3):
        gathered(kind, 0)
    loop(8, 16, hidden)
    gathered(4, 0)

    def down(i):
        both = [span((2 * i + k) * tm, tm) for k in range(2)]
        products = [dot(by_gu[0, rows, :], wd[0]) for rows in both]
        for rows, product in zip(both, products, strict=True):
            h = (xs[rows, :].astype(F32) + product.astype(BF16).astype(F32)).astype(BF16)
            h1[rows, :] = h
            wide = h.astype(F32)
            normed = (wide * scale_of(wide)).astype(BF16)
            a[rows, :] = normed
            at[:, rows] = normed.astype(F32).T.astype(BF16)
        between(2 * i + 16, (16, 18, 20, 22))
        between(2 * i + 17, (17, 19, 21, 23))

    loop(0, 4, down)
    for kind in (0, 1, 4):
        gathered(kind, 1)

    for lam in range(2):
        number = 1 - lam

        def quarter(c, lam=lam, number=number):
            cols = span(c * fc, fc)
            t0 = lam * PERIOD + c * PHASE
            if lam == 0:

                @pl.when(c == CHUNKS // 2)
                def _():
                    for kind in (2, 3):
                        gathered(kind, 1)

            def rows_of(i):
                both = [span((2 * i + k) * tm, tm) for k in range(2)]
                products = [
                    (dot(a[rows, :], wgu[number, 0, :, cols]), dot(a[rows, :], wgu[number, 1, :, cols]), dot_t(do[rows, :], wd[number, cols, :]))
                    for rows in both
                ]
                for rows, (gate, up, by_act) in zip(both, products, strict=True):
                    by_act = by_act.astype(BF16).astype(F32)
                    sig = sigmoid(gate)
                    silu = gate * sig
                    act[rows, :] = (silu * up).astype(BF16)
                    by_gu[1, rows, cols] = (by_act * silu).astype(BF16)
                    by_gu[0, rows, cols] = (by_act * up * (sig + silu * (1.0 - sig))).astype(BF16)
                tick(t0 + i)
                if lam == 0:
                    between(t0 + i + 24, range(24, 28), range(32, 36))

            loop(0, 4, rows_of)
            gu[lam, 0, :, cols] = dot(at[...], by_gu[0, :, cols]).astype(BF16)
            tick(t0 + 4)
            gu[lam, 1, :, cols] = dot(at[...], by_gu[1, :, cols]).astype(BF16)
            tick(t0 + 5)

            def by_down(i):
                rows = span(i * rows_d, rows_d)
                gd[lam, rows, cols] = dot(dot_do[rows, :], act[...]).astype(BF16)
                tick(t0 + 6 + i)
                if lam == 0:
                    between(t0 + i + 30, range(30, 32), range(38, 40))

            loop(0, 2, by_down)

        loop(0, CHUNKS, quarter)

        if lam == 0:
            t0 = CHUNKS * PHASE

            def by_input(i, number=number, t0=t0):
                rows = span(i * tm, tm)
                by_a = dot_t(by_gu[0, rows, :], wgu[number, 0]) + dot_t(by_gu[1, rows, :], wgu[number, 1])
                by_a = by_a.astype(BF16).astype(F32)
                wide = h1[rows, :].astype(F32)
                scale = scale_of(wide)
                inner = jnp.mean(by_a * wide, -1, keepdims=True)
                by_h = (by_a * scale - wide * (scale * scale * scale * inner)).astype(BF16).astype(F32)
                by_h = (do[rows, :].astype(F32) + by_h).astype(BF16)
                do[rows, :] = by_h
                dot_do[:, rows] = by_h.astype(F32).T.astype(BF16)
                wide = xs[rows, :].astype(F32)
                normed = (wide * scale_of(wide)).astype(BF16)
                a[rows, :] = normed
                at[:, rows] = normed.astype(F32).T.astype(BF16)
                tick(t0 + i)

            loop(0, 8, by_input)

    loop(PERIOD + CHUNKS * PHASE, PERIOD + CHUNKS * PHASE + 4 * SPACING + 2, tick)

    outs = []
    for lam in range(2):
        for kind, out in enumerate((g_out, u_out)):
            own = gu.at[lam, kind, span(me * own_d, own_d), :]
            outs.append(pltpu.make_async_copy(own, out.at[1 - lam], out_sem.at[lam, kind]))
        outs.append(pltpu.make_async_copy(d_own.at[lam], d_out.at[1 - lam], out_sem.at[lam, 2]))
    for out in outs:
        out.start()
    lanes = all_squares.shape[2]
    tile = sum(squares_gu[:, i * lanes : (i + 1) * lanes] for i in range(fc // lanes))
    tile = tile + sum(squares_gd[:, i * lanes : (i + 1) * lanes] for i in range(own_f // lanes))
    all_squares[me] = tile
    copies = [
        pltpu.make_async_remote_copy(
            src_ref=all_squares.at[me],
            dst_ref=all_squares.at[me],
            send_sem=sq_send.at[k - 1],
            recv_sem=sq_recv.at[k - 1],
            device_id={"dp": around(k)},
            device_id_type=MESH,
        )
        for k in range(1, n)
    ]
    for copy in copies:
        copy.start()
    for copy in copies:
        copy.wait()
    total = jnp.sum(all_squares[...])
    count = n * (g_out.size + u_out.size + d_out.size)
    factor_out[...] = jnp.minimum(1.0, 0.5 * lax.rsqrt(jnp.full(factor_out.shape, total, F32) / count + 1e-30))
    for kind in range(5):
        for number in range(2):
            await_eighths(kind, number, 56, ag_send.at[kind, number])
    for out in outs:
        out.wait()


def adamw(w, m, v, g):
    m = 0.9 * m + 0.1 * g
    v = 0.95 * v + 0.05 * g * g
    step = m * lax.rsqrt(v + 1e-8) + 0.1 * w
    return (w - 0.02 * step).astype(jnp.bfloat16), m, v


def update(factor, *refs):
    ins, outs = refs[:12], refs[12:]
    for i in range(3):
        w, m, v, g = (ins[3 * k + i] for k in range(4))
        new = adamw(w[...].astype(F32), m[...], v[...], g[...].astype(F32) * factor[0, 0])
        for k in range(3):
            outs[3 * k + i][...] = new[k]


def solution(mesh):
    n, groups = mesh.shape["dp"], mesh.shape["rep"]
    across = math.isqrt(groups // 2)

    def step(x, dy, *arrays):
        weights, m, v = (arrays[i : i + 3] for i in (0, 3, 6))
        layers, own_d, ff = weights[0].shape
        own_f, d = weights[2].shape[1:]
        tokens = x.shape[1]
        fc = ff // CHUNKS
        lanes = min(128, own_f)
        anywhere = pl.BlockSpec(memory_space=pl.ANY)
        *gradients, factor = pl.pallas_call(
            functools.partial(kernel, n, across),
            out_shape=(
                jax.ShapeDtypeStruct((layers, own_d, ff), BF16),
                jax.ShapeDtypeStruct((layers, own_d, ff), BF16),
                jax.ShapeDtypeStruct((layers, own_f, d), BF16),
                jax.ShapeDtypeStruct((8, lanes), F32),
            ),
            in_specs=[anywhere] * 5,
            out_specs=(anywhere, anywhere, anywhere, pl.BlockSpec(memory_space=pltpu.VMEM)),
            scratch_shapes=[
                pltpu.VMEM((layers, 2, d, ff), BF16),
                pltpu.VMEM((layers, ff, d), BF16),
                pltpu.VMEM((layers, 2, d, ff), BF16),
                pltpu.VMEM((layers, d, ff), BF16),
                pltpu.VMEM((CHUNKS, 2, 2, 7 * own_d // 2, fc), BF16),
                pltpu.VMEM((2, 2, 7 * d // 4, own_f), BF16),
                pltpu.VMEM((tokens, d), BF16),
                pltpu.VMEM((tokens, d), BF16),
                pltpu.VMEM((tokens, d), BF16),
                pltpu.VMEM((tokens, d), BF16),
                pltpu.VMEM((d, tokens), BF16),
                pltpu.VMEM((d, tokens), BF16),
                pltpu.VMEM((tokens, fc), BF16),
                pltpu.VMEM((2, tokens, ff), BF16),
                pltpu.VMEM((layers, own_f, d), BF16),
                pltpu.VMEM((8, fc), F32),
                pltpu.VMEM((8, own_f), F32),
                pltpu.VMEM((n, 8, lanes), F32),
                pltpu.SemaphoreType.DMA((2, 4)),
                pltpu.SemaphoreType.DMA((2, 3)),
                pltpu.SemaphoreType.DMA((5, 2)),
                pltpu.SemaphoreType.DMA((5, 2, 4)),
                pltpu.SemaphoreType.DMA((5, 2, 4)),
                pltpu.SemaphoreType.DMA((5, 2)),
                pltpu.SemaphoreType.DMA((CHUNKS + 2, 2)),
                pltpu.SemaphoreType.DMA((CHUNKS + 2, 2, 4)),
                pltpu.SemaphoreType.DMA((n - 1,)),
                pltpu.SemaphoreType.DMA((n - 1,)),
            ],
            compiler_params=pltpu.CompilerParams(collective_id=0, has_side_effects=True, vmem_limit_bytes=67043328),
            name="train_step",
        )(x, dy, *weights)
        pieces = 2

        def blocks(arrays):
            return tuple(
                pl.BlockSpec((1, one.shape[1] // pieces, one.shape[2]), lambda layer, piece: (layer, piece, 0)) for one in arrays
            )

        shapes = [jax.ShapeDtypeStruct(one.shape, kind) for kind in (BF16, F32, F32) for one in weights]
        inputs = (*weights, *m, *v, *gradients)
        return pl.pallas_call(
            update,
            grid=(layers, pieces),
            out_shape=tuple(shapes),
            in_specs=[pl.BlockSpec(memory_space=pltpu.SMEM), *blocks(inputs)],
            out_specs=blocks(shapes),
            name="adamw",
        )(factor, *inputs)

    states, cut = P(("rep", "dp"), None, None), P(None, "dp", None)
    return jax.shard_map(
        step,
        mesh=mesh,
        in_specs=(states, states) + (cut,) * 9,
        out_specs=(P("rep", "dp", None),) * 9,
        check_vma=False,
    )
```
